256 devices in a mesh: crow: 8 (over z_lo, y), ccol: 16 (over z_hi, x), half: 2 (over core).
Axes of the slice: x: 4, y: 4, z: 8 (z_hi: 4, z_lo: 2; z = z_hi * 2 + z_lo), core: 2. Of those that a mesh axis runs over, the one named last changes fastest.
Arguments:
- operator: bfloat16 [8, 16, 2048, 2048], P('crow', 'ccol', 'half'), may hold values from -0.09375 to 0.09375
- east_sources: bfloat16 [8, 16, 384, 2048], P('crow', 'ccol', None, 'half'), may hold values from -6 to 6
- west_sources: bfloat16 [8, 16, 384, 2048], P('crow', 'ccol', None, 'half'), may hold values from -6 to 6
Outputs:
- east_traces: bfloat16 [8, 16, 384, 2048], P('crow', 'ccol', None, 'half')
- west_traces: bfloat16 [8, 16, 384, 2048], P('crow', 'ccol', None, 'half')
The draws below stay inside these ranges and needn't reach their ends.
All inputs are finite; a program needn't handle non-finite values.
Results may differ from the reference program's by a relative error of at most 0.025.
Values may be sent and summed in bfloat16 or wider, within the bound.
No kernel may reach another device: no remote copies, remote signals or barrier semaphores. Data moves between devices by JAX's collectives and lax.ppermute only.
A program may use at most 64 MiB of HBM per device.

```python
import jax
import jax.numpy as jnp
from jax import lax

TRACE = 2048
BATCH = 384
CELL_ROWS = 8
CELL_COLS = 16


def shard_levels(stream_key, dims, shards, least, top_value):
    gain, own = 1.0, jax.random.fold_in(stream_key, 6)
    for dim, blocks in shards:
        draws = jnp.exp(jax.random.uniform(jax.random.fold_in(own, dim), (blocks,), jnp.float32, least / len(shards), top_value / len(shards)))
        gain = gain * jnp.repeat(draws, dims[dim] // blocks).reshape([-1 if axis == dim else 1 for axis in range(len(dims))])
    return gain


def centred(stream_key, shape, deviation, bound, shards=(), kind=jnp.bfloat16):
    factor_of = shard_levels(stream_key, shape, shards, -0.22, 0.18) if shards else 1.0
    drawn = jax.random.normal(stream_key, shape, jnp.float32) * deviation * factor_of
    return jnp.minimum(jnp.maximum(drawn, -bound), bound).astype(kind)


def setup_inputs(seed: int = 0) -> dict:
    key_of = jax.random.split(jax.random.key(seed), 4)
    return {
        "operator": centred(key_of[0], (CELL_ROWS, CELL_COLS, TRACE, TRACE), (2 * TRACE) ** -0.5, 0.09375, ((0, 8), (1, 16), (2, 2))),
        "east_sources": centred(key_of[1], (CELL_ROWS, CELL_COLS, BATCH, TRACE), 1.0, 6.0, ((0, 8), (1, 16), (3, 2))),
        "west_sources": centred(key_of[2], (CELL_ROWS, CELL_COLS, BATCH, TRACE), 1.0, 6.0, ((0, 8), (1, 16), (3, 2))),
    }


def sweep_one(operator, sources, transpose):
    cols_total = operator.shape[1]
    batch_rows = sources.shape[2]
    trace_width = sources.shape[3]

    def row_step(upper_row, row_inputs):
        op_row, source_row = row_inputs

        def cell_step(western, inputs):
            matrix, source, from_north = inputs
            inflow = (from_north.astype(jnp.float32) + western.astype(jnp.float32)).astype(jnp.bfloat16)
            inflow = lax.optimization_barrier(inflow).astype(jnp.float32)
            dense = matrix.astype(jnp.float32)
            if transpose:
                dense = dense.T
            product = jnp.dot(inflow, dense, precision=lax.Precision.HIGHEST)
            newest = (product + source.astype(jnp.float32)).astype(jnp.bfloat16)
            return newest, newest

        start_west = jnp.zeros((batch_rows, trace_width), jnp.bfloat16)
        _, row_out = lax.scan(cell_step, start_west, (op_row, source_row, upper_row))
        return row_out, row_out

    start_row = jnp.zeros((cols_total, batch_rows, trace_width), jnp.bfloat16)
    _, traces = lax.scan(row_step, start_row, (operator, sources))
    return traces


def reference(operator, east_sources, west_sources):
    east_traces = sweep_one(operator, east_sources, True)
    flipped_op = jnp.flip(operator, axis=(0, 1))
    flipped_src = jnp.flip(west_sources, axis=(0, 1))
    west_traces = jnp.flip(sweep_one(flipped_op, flipped_src, False), axis=(0, 1))
    return east_traces, west_traces
```

```python
import functools

import jax
import jax.numpy as jnp
from jax import lax
from jax.experimental import pallas as pl
from jax.experimental.pallas import tpu as pltpu
from jax.sharding import PartitionSpec as P

BLOCKS = 8
RING = 4
VMEM_LIMIT = 24 << 20


def position():
    half = lax.axis_index("half")
    row = lax.axis_index("crow")
    col = lax.axis_index("ccol")
    row = jnp.where(half == 0, row, lax.axis_size("crow") - 1 - row)
    col = jnp.where(half == 0, col, lax.axis_size("ccol") - 1 - col)
    return half, row, col


def forward_pairs(length, edges):
    pairs = []
    for a, b in edges:
        pairs.append((2 * a, 2 * b))
        pairs.append((2 * (length - 1 - a) + 1, 2 * (length - 1 - b) + 1))
    return pairs


def ring_edges(length):
    return [(i, i // RING * RING + (i + 1) % RING) for i in range(length)]


def long_edges(length):
    return [(i, i + 1) for i in range(RING - 1, length - 1, RING)]


def swap(x):
    return lax.ppermute(x, "half", [(0, 1), (1, 0)])


def prepare_kernel(own_ref, other_ref, out_ref):
    half = lax.axis_index("half")
    rows, width = own_ref.shape
    chunk = 256

    @pl.when(half == 0)
    def _():
        for k in range(rows // chunk):
            s = slice(k * chunk, (k + 1) * chunk)
            out_ref[:, s] = own_ref[s, :].T
            out_ref[:, rows + k * chunk : rows + (k + 1) * chunk] = other_ref[s, :].T

    @pl.when(half == 1)
    def _():
        out_ref[:rows, :] = other_ref[...]
        out_ref[rows:, :] = own_ref[...]


def prepare(own, other):
    rows, width = own.shape
    vmem = pl.BlockSpec(memory_space=pltpu.VMEM)
    return pl.pallas_call(
        prepare_kernel,
        out_shape=jax.ShapeDtypeStruct((2 * rows, width), own.dtype),
        in_specs=[vmem, vmem],
        out_specs=vmem,
        compiler_params=pltpu.CompilerParams(vmem_limit_bytes=VMEM_LIMIT),
        cost_estimate=pl.CostEstimate(flops=0, bytes_accessed=4 * rows * width * 2, transcendentals=0),
        name="prepare",
    )(own, other)


def step_kernel(step, block_count, *refs):
    (ring_n, ring_w, long_n, long_w, matrix, src_own, src_other, _, _, newest, kept, sent) = refs
    half, row, col = position()
    level = row + col + row // RING + col // RING
    block = step - level
    rows, width = newest.shape
    mid = width // 2

    @pl.when((block >= 0) & (block < block_count))
    def _():
        at = pl.ds(pl.multiple_of(block * rows, rows), rows)
        zero = jnp.zeros((rows, width), jnp.float32)
        north = jnp.where(row == 0, zero, jnp.where(row % RING == 0, long_n[...], ring_n[...]).astype(jnp.float32))
        west = jnp.where(col == 0, zero, jnp.where(col % RING == 0, long_w[...], ring_w[...]).astype(jnp.float32))
        inflow = (north + west).astype(jnp.bfloat16)
        own, other = src_own[at, :], src_other[at, :]
        low = jnp.where(half == 0, own, other).astype(jnp.float32)
        high = jnp.where(half == 0, other, own).astype(jnp.float32)
        low = (jnp.dot(inflow, matrix[:, :mid], preferred_element_type=jnp.float32) + low).astype(jnp.bfloat16)
        newest[:, :mid] = low
        high = (jnp.dot(inflow, matrix[:, mid:], preferred_element_type=jnp.float32) + high).astype(jnp.bfloat16)
        newest[:, mid:] = high
        kept[at, :] = jnp.where(half == 0, low, high)
        sent[at, :] = jnp.where(half == 0, high, low)


def run_step(step, rows, matrix, inflows, sources, results):
    block_count = sources[0].shape[0] // rows
    width = matrix.shape[1]
    vmem = pl.BlockSpec(memory_space=pltpu.VMEM)
    outs = [jax.ShapeDtypeStruct((rows, width), jnp.bfloat16)]
    outs += [jax.ShapeDtypeStruct(r.shape, r.dtype) for r in results]
    return pl.pallas_call(
        functools.partial(step_kernel, step, block_count),
        out_shape=outs,
        in_specs=[vmem] * 9,
        out_specs=[vmem] * 3,
        input_output_aliases={7: 1, 8: 2},
        compiler_params=pltpu.CompilerParams(vmem_limit_bytes=VMEM_LIMIT),
        cost_estimate=pl.CostEstimate(flops=2 * rows * width * width, bytes_accessed=width * width * 2, transcendentals=0),
        name="cell_step",
    )(*inflows, matrix, *sources, *results)


def local(operator, east_sources, west_sources):
    matrix = operator[0, 0]
    east, west = east_sources[0, 0], west_sources[0, 0]
    batch, half_width = east.shape
    width = matrix.shape[1]
    rows = batch // BLOCKS
    crow, ccol = lax.axis_size("crow"), lax.axis_size("ccol")
    first = lax.axis_index("half") == 0
    src_own = jnp.where(first, east, west)
    src_other = swap(jnp.where(first, west, east))
    whole = prepare(matrix, swap(matrix))

    ring_row = lambda x: lax.ppermute(x, ("crow", "half"), forward_pairs(crow, ring_edges(crow)))
    ring_col = lambda x: lax.ppermute(x, ("ccol", "half"), forward_pairs(ccol, ring_edges(ccol)))
    long_row = lambda x: lax.ppermute(x, ("crow", "half"), forward_pairs(crow, long_edges(crow)))
    long_col = lambda x: lax.ppermute(x, ("ccol", "half"), forward_pairs(ccol, long_edges(ccol)))

    empty = jnp.zeros((rows, width), jnp.bfloat16)
    results = [jnp.zeros((batch, half_width), jnp.bfloat16)] * 2
    top = lambda length: (length - 1) + (length - 1) // RING
    last_level = top(crow) + top(ccol)
    steps = last_level + BLOCKS
    row_sends = range(RING - 1, (crow - RING - 1) + (crow // RING - 2) + top(ccol) + BLOCKS)
    col_sends = range(RING - 1, (ccol - RING - 1) + (ccol // RING - 2) + top(crow) + BLOCKS)
    ring_n = ring_w = empty
    later_n, later_w = empty, empty
    for step in range(steps):
        long_n, long_w = later_n, later_w
        newest, *results = run_step(step, rows, whole, (ring_n, ring_w, long_n, long_w), (src_own, src_other), results)
        if step == steps - 1:
            break
        ring_n, ring_w = ring_row(newest), ring_col(newest)
        if step > 0:
            later_n, later_w = pending_n, pending_w
        pending_n = long_row(newest) if step in row_sends else empty
        pending_w = long_col(newest) if step in col_sends else empty
    kept, sent = results
    back = swap(sent)
    east_out = jnp.where(first, kept, back)
    west_out = jnp.where(first, back, kept)
    return east_out[None, None], west_out[None, None]


def solution(mesh):
    in_specs = (
        P("crow", "ccol", "half", None),
        P("crow", "ccol", None, "half"),
        P("crow", "ccol", None, "half"),
    )
    out_specs = (P("crow", "ccol", None, "half"), P("crow", "ccol", None, "half"))
    return jax.shard_map(local, mesh=mesh, in_specs=in_specs, out_specs=out_specs, check_vma=False)
```

```python
import functools

import jax
import jax.numpy as jnp
from jax import lax
from jax.experimental import pallas as pl
from jax.experimental.pallas import tpu as pltpu
from jax.sharding import PartitionSpec as P

BLOCKS = 8
RING = 4
VMEM_LIMIT = 24 << 20


def position():
    half = lax.axis_index("half")
    row = lax.axis_index("crow")
    col = lax.axis_index("ccol")
    row = jnp.where(half == 0, row, lax.axis_size("crow") - 1 - row)
    col = jnp.where(half == 0, col, lax.axis_size("ccol") - 1 - col)
    return half, row, col


def folded_pairs(length, edges):
    goes = {}
    for a, b in edges:
        goes[2 * a] = 2 * b
        goes[2 * (length - 1 - a) + 1] = 2 * (length - 1 - b) + 1
    for device in range(2 * length):
        goes.setdefault(device, device ^ 1)
    return sorted(goes.items())


def line_edges(length):
    return [(i, i + 1) for i in range(length - 1) if i % RING != RING - 1]


def long_edges(length):
    return [(i, i + 1) for i in range(RING - 1, length - 1, RING)]


def swap(x):
    return lax.ppermute(x, "half", [(0, 1), (1, 0)])


def prepare_kernel(own_ref, other_ref, out_ref):
    half = lax.axis_index("half")
    rows, width = own_ref.shape
    chunk = 256

    @pl.when(half == 0)
    def _():
        for k in range(rows // chunk):
            s = slice(k * chunk, (k + 1) * chunk)
            out_ref[:, s] = own_ref[s, :].T
            out_ref[:, rows + k * chunk : rows + (k + 1) * chunk] = other_ref[s, :].T

    @pl.when(half == 1)
    def _():
        out_ref[:rows, :] = other_ref[...]
        out_ref[rows:, :] = own_ref[...]


def prepare(own, other):
    rows, width = own.shape
    vmem = pl.BlockSpec(memory_space=pltpu.VMEM)
    return pl.pallas_call(
        prepare_kernel,
        out_shape=jax.ShapeDtypeStruct((2 * rows, width), own.dtype),
        in_specs=[vmem, vmem],
        out_specs=vmem,
        compiler_params=pltpu.CompilerParams(vmem_limit_bytes=VMEM_LIMIT),
        cost_estimate=pl.CostEstimate(flops=0, bytes_accessed=4 * rows * width * 2, transcendentals=0),
        name="prepare",
    )(own, other)


def step_kernel(step, block_count, *refs):
    (ring_n, ring_w, long_n, long_w, matrix, src_own, src_other, _, _, newest, kept, sent) = refs
    half, row, col = position()
    level = row + col + row // RING + col // RING
    block = step - level
    rows, width = newest.shape
    mid = width // 2

    @pl.when((block >= 0) & (block < block_count))
    def _():
        at = pl.ds(pl.multiple_of(block * rows, rows), rows)
        zero = jnp.zeros((rows, width), jnp.float32)
        north = jnp.where(row == 0, zero, jnp.where(row % RING == 0, long_n[...], ring_n[...]).astype(jnp.float32))
        west = jnp.where(col == 0, zero, jnp.where(col % RING == 0, long_w[...], ring_w[...]).astype(jnp.float32))
        inflow = (north + west).astype(jnp.bfloat16)
        own, other = src_own[at, :], src_other[at, :]
        low = jnp.where(half == 0, own, other).astype(jnp.float32)
        high = jnp.where(half == 0, other, own).astype(jnp.float32)
        low = (jnp.dot(inflow, matrix[:, :mid], preferred_element_type=jnp.float32) + low).astype(jnp.bfloat16)
        newest[:, :mid] = low
        high = (jnp.dot(inflow, matrix[:, mid:], preferred_element_type=jnp.float32) + high).astype(jnp.bfloat16)
        newest[:, mid:] = high
        kept[at, :] = jnp.where(half == 0, low, high)
        sent[at, :] = jnp.where(half == 0, high, low)


def run_step(step, rows, matrix, inflows, sources, results):
    block_count = sources[0].shape[0] // rows
    width = matrix.shape[1]
    vmem = pl.BlockSpec(memory_space=pltpu.VMEM)
    outs = [jax.ShapeDtypeStruct((rows, width), jnp.bfloat16)]
    outs += [jax.ShapeDtypeStruct(r.shape, r.dtype) for r in results]
    return pl.pallas_call(
        functools.partial(step_kernel, step, block_count),
        out_shape=outs,
        in_specs=[vmem] * 9,
        out_specs=[vmem] * 3,
        input_output_aliases={7: 1, 8: 2},
        compiler_params=pltpu.CompilerParams(vmem_limit_bytes=VMEM_LIMIT),
        cost_estimate=pl.CostEstimate(flops=2 * rows * width * width, bytes_accessed=width * width * 2, transcendentals=0),
        name="cell_step",
    )(*inflows, matrix, *sources, *results)


def local(operator, east_sources, west_sources):
    matrix = operator[0, 0]
    east, west = east_sources[0, 0], west_sources[0, 0]
    batch, half_width = east.shape
    width = matrix.shape[1]
    rows = batch // BLOCKS
    crow, ccol = lax.axis_size("crow"), lax.axis_size("ccol")
    first = lax.axis_index("half") == 0
    src_own = jnp.where(first, east, west)
    src_other = swap(jnp.where(first, west, east))
    whole = prepare(matrix, swap(matrix))

    ring_row = lambda x: lax.ppermute(x, ("crow", "half"), folded_pairs(crow, line_edges(crow)))
    ring_col = lambda x: lax.ppermute(x, ("ccol", "half"), folded_pairs(ccol, line_edges(ccol)))
    long_row = lambda x: lax.ppermute(x, ("crow", "half"), folded_pairs(crow, long_edges(crow)))
    long_col = lambda x: lax.ppermute(x, ("ccol", "half"), folded_pairs(ccol, long_edges(ccol)))

    empty = jnp.zeros((rows, width), jnp.bfloat16)
    results = [jnp.zeros((batch, half_width), jnp.bfloat16)] * 2
    top = lambda length: (length - 1) + (length - 1) // RING
    last_level = top(crow) + top(ccol)
    steps = last_level + BLOCKS
    row_sends = range(RING - 1, (crow - RING - 1) + (crow // RING - 2) + top(ccol) + BLOCKS)
    col_sends = range(RING - 1, (ccol - RING - 1) + (ccol // RING - 2) + top(crow) + BLOCKS)
    ring_n = ring_w = empty
    later_n, later_w = empty, empty
    for step in range(steps):
        long_n, long_w = later_n, later_w
        newest, *results = run_step(step, rows, whole, (ring_n, ring_w, long_n, long_w), (src_own, src_other), results)
        if step == steps - 1:
            break
        ring_n, ring_w = ring_row(newest), ring_col(newest)
        if step > 0:
            later_n, later_w = pending_n, pending_w
        pending_n = long_row(newest) if step in row_sends else empty
        pending_w = long_col(newest) if step in col_sends else empty
    kept, sent = results
    back = swap(sent)
    east_out = jnp.where(first, kept, back)
    west_out = jnp.where(first, back, kept)
    return east_out[None, None], west_out[None, None]


def solution(mesh):
    in_specs = (
        P("crow", "ccol", "half", None),
        P("crow", "ccol", None, "half"),
        P("crow", "ccol", None, "half"),
    )
    out_specs = (P("crow", "ccol", None, "half"), P("crow", "ccol", None, "half"))
    return jax.shard_map(local, mesh=mesh, in_specs=in_specs, out_specs=out_specs, check_vma=False)
```

```python
import functools

import jax
import jax.numpy as jnp
from jax import lax
from jax.experimental import pallas as pl
from jax.experimental.pallas import tpu as pltpu
from jax.sharding import PartitionSpec as P

BLOCKS = 8
CHUNKS = 4
RING = 4
VMEM_LIMIT = 24 << 20


def position():
    half = lax.axis_index("half")
    row = lax.axis_index("crow")
    col = lax.axis_index("ccol")
    row = jnp.where(half == 0, row, lax.axis_size("crow") - 1 - row)
    col = jnp.where(half == 0, col, lax.axis_size("ccol") - 1 - col)
    return half, row, col


def folded_pairs(length, edges):
    goes = {}
    for a, b in edges:
        goes[2 * a] = 2 * b
        goes[2 * (length - 1 - a) + 1] = 2 * (length - 1 - b) + 1
    for device in range(2 * length):
        goes.setdefault(device, device ^ 1)
    return sorted(goes.items())


def line_edges(length):
    return [(i, i + 1) for i in range(length - 1) if i % RING != RING - 1]


def long_edges(length):
    return [(i, i + 1) for i in range(RING - 1, length - 1, RING)]


def swap(x):
    return lax.ppermute(x, "half", [(0, 1), (1, 0)])


def prepare_kernel(mine, rows_ref, *refs):
    out_ref, held, sems = refs[-3:]
    half = lax.axis_index("half")
    rows = rows_ref.shape[0]
    chunk = rows // CHUNKS

    @pl.when(half == 0)
    def _():
        copies = [
            pltpu.make_async_copy(rows_ref.at[pl.ds(k * chunk, chunk), :], held.at[k], sems.at[k]) for k in range(CHUNKS)
        ]
        for copy in copies:
            copy.start()
        first = 0 if mine else rows
        for k, copy in enumerate(copies):
            copy.wait()
            out_ref[:, first + k * chunk : first + (k + 1) * chunk] = held[k].T

    @pl.when(half == 1)
    def _():
        first = rows if mine else 0
        copy = pltpu.make_async_copy(rows_ref, out_ref.at[pl.ds(first, rows), :], sems.at[CHUNKS])
        copy.start()
        copy.wait()


def prepare(mine, half_matrix, *whole):
    rows, width = half_matrix.shape
    return pl.pallas_call(
        functools.partial(prepare_kernel, mine),
        out_shape=jax.ShapeDtypeStruct((2 * rows, width), half_matrix.dtype),
        in_specs=[pl.BlockSpec(memory_space=pltpu.HBM)] + [pl.BlockSpec(memory_space=pltpu.VMEM)] * len(whole),
        out_specs=pl.BlockSpec(memory_space=pltpu.VMEM),
        scratch_shapes=[
            pltpu.VMEM((CHUNKS, rows // CHUNKS, width), half_matrix.dtype),
            pltpu.SemaphoreType.DMA((CHUNKS + 1,)),
        ],
        input_output_aliases={1: 0} if whole else {},
        compiler_params=pltpu.CompilerParams(vmem_limit_bytes=24 << 20),
        cost_estimate=pl.CostEstimate(flops=0, bytes_accessed=4 * rows * width, transcendentals=0),
        name="prepare",
    )(half_matrix, *whole)


def first_kernel(rows, src_own, src_other, newest, kept, sent):
    half, row, col = position()
    mid = newest.shape[1] // 2

    @pl.when((row == 0) & (col == 0))
    def _():
        own, other = src_own[:rows, :], src_other[:rows, :]
        newest[:, :mid] = jnp.where(half == 0, own, other)
        newest[:, mid:] = jnp.where(half == 0, other, own)
        kept[:rows, :] = own
        sent[:rows, :] = other


def first_step(rows, first_sources, sources):
    vmem = pl.BlockSpec(memory_space=pltpu.VMEM)
    batch, half_width = sources[0].shape
    shapes = [(rows, 2 * half_width), (batch, half_width), (batch, half_width)]
    return pl.pallas_call(
        functools.partial(first_kernel, rows),
        out_shape=[jax.ShapeDtypeStruct(shape, jnp.bfloat16) for shape in shapes],
        in_specs=[vmem] * 2,
        out_specs=[vmem] * 3,
        compiler_params=pltpu.CompilerParams(vmem_limit_bytes=VMEM_LIMIT),
        cost_estimate=pl.CostEstimate(flops=0, bytes_accessed=rows * half_width * 8, transcendentals=0),
        name="first_step",
    )(*first_sources)


def step_kernel(step, block_count, *refs):
    (ring_n, ring_w, long_n, long_w, matrix, src_own, src_other, _, _, newest, kept, sent) = refs
    half, row, col = position()
    level = row + col + row // RING + col // RING
    block = step - level
    rows, width = newest.shape
    mid = width // 2

    @pl.when((block >= 0) & (block < block_count))
    def _():
        at = pl.ds(pl.multiple_of(block * rows, rows), rows)
        zero = jnp.zeros((rows, width), jnp.float32)
        north = jnp.where(row == 0, zero, jnp.where(row % RING == 0, long_n[...], ring_n[...]).astype(jnp.float32))
        west = jnp.where(col == 0, zero, jnp.where(col % RING == 0, long_w[...], ring_w[...]).astype(jnp.float32))
        inflow = (north + west).astype(jnp.bfloat16)
        own, other = src_own[at, :], src_other[at, :]
        low = jnp.where(half == 0, own, other).astype(jnp.float32)
        high = jnp.where(half == 0, other, own).astype(jnp.float32)
        low = (jnp.dot(inflow, matrix[:, :mid], preferred_element_type=jnp.float32) + low).astype(jnp.bfloat16)
        newest[:, :mid] = low
        high = (jnp.dot(inflow, matrix[:, mid:], preferred_element_type=jnp.float32) + high).astype(jnp.bfloat16)
        newest[:, mid:] = high
        kept[at, :] = jnp.where(half == 0, low, high)
        sent[at, :] = jnp.where(half == 0, high, low)


def run_step(step, rows, matrix, inflows, sources, results):
    block_count = sources[0].shape[0] // rows
    width = matrix.shape[1]
    vmem = pl.BlockSpec(memory_space=pltpu.VMEM)
    outs = [jax.ShapeDtypeStruct((rows, width), jnp.bfloat16)]
    outs += [jax.ShapeDtypeStruct(r.shape, r.dtype) for r in results]
    return pl.pallas_call(
        functools.partial(step_kernel, step, block_count),
        out_shape=outs,
        in_specs=[vmem] * 9,
        out_specs=[vmem] * 3,
        input_output_aliases={7: 1, 8: 2},
        compiler_params=pltpu.CompilerParams(vmem_limit_bytes=VMEM_LIMIT),
        cost_estimate=pl.CostEstimate(flops=2 * rows * width * width, bytes_accessed=width * width * 2, transcendentals=0),
        name="cell_step",
    )(*inflows, matrix, *sources, *results)


def local(operator, east_sources, west_sources):
    matrix = operator[0, 0]
    east, west = east_sources[0, 0], west_sources[0, 0]
    batch, half_width = east.shape
    width = matrix.shape[1]
    rows = batch // BLOCKS
    crow, ccol = lax.axis_size("crow"), lax.axis_size("ccol")
    first = lax.axis_index("half") == 0
    first_other = swap(jnp.where(first, west[:rows], east[:rows]))
    first_own = jnp.where(first, east[:rows], west[:rows])
    first_other, matrix, east, west = lax.optimization_barrier((first_other, matrix, east, west))
    other_half = swap(matrix)
    sources = (jnp.where(first, east, west), swap(jnp.where(first, west, east)))
    whole = prepare(True, matrix)

    ring_row = lambda x: lax.ppermute(x, ("crow", "half"), folded_pairs(crow, line_edges(crow)))
    ring_col = lambda x: lax.ppermute(x, ("ccol", "half"), folded_pairs(ccol, line_edges(ccol)))
    long_row = lambda x: lax.ppermute(x, ("crow", "half"), folded_pairs(crow, long_edges(crow)))
    long_col = lambda x: lax.ppermute(x, ("ccol", "half"), folded_pairs(ccol, long_edges(ccol)))

    empty = jnp.zeros((rows, width), jnp.bfloat16)
    top = lambda length: (length - 1) + (length - 1) // RING
    last_level = top(crow) + top(ccol)
    steps = last_level + BLOCKS
    row_sends = range(RING - 1, (crow - RING - 1) + (crow // RING - 2) + top(ccol) + BLOCKS)
    col_sends = range(RING - 1, (ccol - RING - 1) + (ccol // RING - 2) + top(crow) + BLOCKS)
    ring_n = ring_w = empty
    later_n, later_w = empty, empty
    for step in range(steps):
        long_n, long_w = later_n, later_w
        if step == 0:
            newest, *results = first_step(rows, (first_own, first_other), sources)
        else:
            if step == 1:
                whole = prepare(False, other_half, whole)
            newest, *results = run_step(step, rows, whole, (ring_n, ring_w, long_n, long_w), sources, results)
        if step == steps - 1:
            break
        ring_n, ring_w = ring_row(newest), ring_col(newest)
        if step > 0:
            later_n, later_w = pending_n, pending_w
        pending_n = long_row(newest) if step in row_sends else empty
        pending_w = long_col(newest) if step in col_sends else empty
    kept, sent = results
    back = swap(sent)
    east_out = jnp.where(first, kept, back)
    west_out = jnp.where(first, back, kept)
    return east_out[None, None], west_out[None, None]


def solution(mesh):
    in_specs = (
        P("crow", "ccol", "half", None),
        P("crow", "ccol", None, "half"),
        P("crow", "ccol", None, "half"),
    )
    out_specs = (P("crow", "ccol", None, "half"), P("crow", "ccol", None, "half"))
    return jax.shard_map(local, mesh=mesh, in_specs=in_specs, out_specs=out_specs, check_vma=False)
```

```python
import functools

import jax
import jax.numpy as jnp
from jax import lax
from jax.experimental import pallas as pl
from jax.experimental.pallas import tpu as pltpu
from jax.sharding import PartitionSpec as P

BLOCKS = 8
CHUNKS = 4
RING = 4
VMEM_LIMIT = 24 << 20


def position():
    half = lax.axis_index("half")
    row = lax.axis_index("crow")
    col = lax.axis_index("ccol")
    row = jnp.where(half == 0, row, lax.axis_size("crow") - 1 - row)
    col = jnp.where(half == 0, col, lax.axis_size("ccol") - 1 - col)
    return half, row, col


def folded_pairs(length, edges):
    goes = {}
    for a, b in edges:
        goes[2 * a] = 2 * b
        goes[2 * (length - 1 - a) + 1] = 2 * (length - 1 - b) + 1
    for device in range(2 * length):
        goes.setdefault(device, device ^ 1)
    return sorted(goes.items())


def line_edges(length):
    return [(i, i + 1) for i in range(length - 1) if i % RING != RING - 1]


def long_edges(length):
    return [(i, i + 1) for i in range(RING - 1, length - 1, RING)]


def swap(x):
    return lax.ppermute(x, "half", [(0, 1), (1, 0)])


def prepare_kernel(mine, rows_ref, *refs):
    out_ref, held, sems = refs[-3:]
    half = lax.axis_index("half")
    rows = rows_ref.shape[0]
    chunk = rows // CHUNKS

    @pl.when(half == 0)
    def _():
        copies = [
            pltpu.make_async_copy(rows_ref.at[pl.ds(k * chunk, chunk), :], held.at[k], sems.at[k]) for k in range(CHUNKS)
        ]
        for copy in copies:
            copy.start()
        first = 0 if mine else rows
        for k, copy in enumerate(copies):
            copy.wait()
            out_ref[:, first + k * chunk : first + (k + 1) * chunk] = held[k].T

    @pl.when(half == 1)
    def _():
        first = rows if mine else 0
        copy = pltpu.make_async_copy(rows_ref, out_ref.at[pl.ds(first, rows), :], sems.at[CHUNKS])
        copy.start()
        copy.wait()


def prepare(mine, half_matrix, *whole):
    rows, width = half_matrix.shape
    return pl.pallas_call(
        functools.partial(prepare_kernel, mine),
        out_shape=jax.ShapeDtypeStruct((2 * rows, width), half_matrix.dtype),
        in_specs=[pl.BlockSpec(memory_space=pltpu.HBM)] + [pl.BlockSpec(memory_space=pltpu.VMEM)] * len(whole),
        out_specs=pl.BlockSpec(memory_space=pltpu.VMEM),
        scratch_shapes=[
            pltpu.VMEM((CHUNKS, rows // CHUNKS, width), half_matrix.dtype),
            pltpu.SemaphoreType.DMA((CHUNKS + 1,)),
        ],
        input_output_aliases={1: 0} if whole else {},
        compiler_params=pltpu.CompilerParams(vmem_limit_bytes=24 << 20),
        cost_estimate=pl.CostEstimate(flops=0, bytes_accessed=4 * rows * width, transcendentals=0),
        name="prepare",
    )(half_matrix, *whole)


def first_kernel(rows, src_own, src_other, newest, kept, sent):
    half, row, col = position()
    mid = newest.shape[1] // 2

    @pl.when((row == 0) & (col == 0))
    def _():
        own, other = src_own[:rows, :], src_other[:rows, :]
        newest[:, :mid] = jnp.where(half == 0, own, other)
        newest[:, mid:] = jnp.where(half == 0, other, own)
        kept[:rows, :] = own
        sent[:rows, :] = other


def first_step(rows, first_sources, sources):
    vmem = pl.BlockSpec(memory_space=pltpu.VMEM)
    batch, half_width = sources[0].shape
    shapes = [(rows, 2 * half_width), (batch, half_width), (batch, half_width)]
    return pl.pallas_call(
        functools.partial(first_kernel, rows),
        out_shape=[jax.ShapeDtypeStruct(shape, jnp.bfloat16) for shape in shapes],
        in_specs=[vmem] * 2,
        out_specs=[vmem] * 3,
        compiler_params=pltpu.CompilerParams(vmem_limit_bytes=VMEM_LIMIT),
        cost_estimate=pl.CostEstimate(flops=0, bytes_accessed=rows * half_width * 8, transcendentals=0),
        name="first_step",
    )(*first_sources)


def step_kernel(step, block_count, last, *refs):
    if last:
        (ring_n, ring_w, long_n, long_w, matrix, src_own, src_other, _, sent, kept, final) = refs
        newest = None
    else:
        (ring_n, ring_w, long_n, long_w, matrix, src_own, src_other, _, _, newest, kept, sent) = refs
    half, row, col = position()
    level = row + col + row // RING + col // RING
    block = step - level
    rows, width = ring_n.shape
    mid = width // 2

    if last:
        final[...] = sent[sent.shape[0] - rows :, :]

    @pl.when((block >= 0) & (block < block_count))
    def _():
        at = pl.ds(pl.multiple_of(block * rows, rows), rows)
        zero = jnp.zeros((rows, width), jnp.float32)
        north = jnp.where(row == 0, zero, jnp.where(row % RING == 0, long_n[...], ring_n[...]).astype(jnp.float32))
        west = jnp.where(col == 0, zero, jnp.where(col % RING == 0, long_w[...], ring_w[...]).astype(jnp.float32))
        inflow = (north + west).astype(jnp.bfloat16)
        own, other = src_own[at, :], src_other[at, :]
        low = jnp.where(half == 0, own, other).astype(jnp.float32)
        high = jnp.where(half == 0, other, own).astype(jnp.float32)
        low = (jnp.dot(inflow, matrix[:, :mid], preferred_element_type=jnp.float32) + low).astype(jnp.bfloat16)
        if not last:
            newest[:, :mid] = low
        high = (jnp.dot(inflow, matrix[:, mid:], preferred_element_type=jnp.float32) + high).astype(jnp.bfloat16)
        kept[at, :] = jnp.where(half == 0, low, high)
        given = jnp.where(half == 0, high, low)
        if last:
            final[...] = given
        else:
            newest[:, mid:] = high
            sent[at, :] = given


def run_step(step, rows, matrix, inflows, sources, results, last):
    block_count = sources[0].shape[0] // rows
    width = matrix.shape[1]
    vmem = pl.BlockSpec(memory_space=pltpu.VMEM)
    kept, sent = [jax.ShapeDtypeStruct(r.shape, r.dtype) for r in results]
    if last:
        outs = [kept, jax.ShapeDtypeStruct((rows, width // 2), jnp.bfloat16)]
    else:
        outs = [jax.ShapeDtypeStruct((rows, width), jnp.bfloat16), kept, sent]
    return pl.pallas_call(
        functools.partial(step_kernel, step, block_count, last),
        out_shape=outs,
        in_specs=[vmem] * 9,
        out_specs=[vmem] * len(outs),
        input_output_aliases={7: 0} if last else {7: 1, 8: 2},
        compiler_params=pltpu.CompilerParams(vmem_limit_bytes=VMEM_LIMIT),
        cost_estimate=pl.CostEstimate(flops=2 * rows * width * width, bytes_accessed=width * width * 2, transcendentals=0),
        name="cell_step",
    )(*inflows, matrix, *sources, *results)


def local(operator, east_sources, west_sources):
    matrix = operator[0, 0]
    east, west = east_sources[0, 0], west_sources[0, 0]
    batch, half_width = east.shape
    width = matrix.shape[1]
    rows = batch // BLOCKS
    crow, ccol = lax.axis_size("crow"), lax.axis_size("ccol")
    first = lax.axis_index("half") == 0
    first_other = swap(jnp.where(first, west[:rows], east[:rows]))
    first_own = jnp.where(first, east[:rows], west[:rows])
    first_other, matrix, east, west = lax.optimization_barrier((first_other, matrix, east, west))
    other_half = swap(matrix)
    sources = (jnp.where(first, east, west), swap(jnp.where(first, west, east)))
    whole = prepare(True, matrix)

    ring_row = lambda x: lax.ppermute(x, ("crow", "half"), folded_pairs(crow, line_edges(crow)))
    ring_col = lambda x: lax.ppermute(x, ("ccol", "half"), folded_pairs(ccol, line_edges(ccol)))
    long_row = lambda x: lax.ppermute(x, ("crow", "half"), folded_pairs(crow, long_edges(crow)))
    long_col = lambda x: lax.ppermute(x, ("ccol", "half"), folded_pairs(ccol, long_edges(ccol)))

    empty = jnp.zeros((rows, width), jnp.bfloat16)
    top = lambda length: (length - 1) + (length - 1) // RING
    last_level = top(crow) + top(ccol)
    steps = last_level + BLOCKS
    row_sends = range(RING - 1, (crow - RING - 1) + (crow // RING - 2) + top(ccol) + BLOCKS)
    col_sends = range(RING - 1, (ccol - RING - 1) + (ccol // RING - 2) + top(crow) + BLOCKS)
    ring_n = ring_w = empty
    later_n, later_w = empty, empty
    for step in range(steps):
        long_n, long_w = later_n, later_w
        if step == 0:
            newest, *results = first_step(rows, (first_own, first_other), sources)
        else:
            if step == 1:
                whole = prepare(False, other_half, whole)
            last = step == steps - 1
            if last:
                back = swap(results[1])
            outs = run_step(step, rows, whole, (ring_n, ring_w, long_n, long_w), sources, results, last)
            if last:
                kept, final = outs
                break
            newest, *results = outs
        ring_n, ring_w = ring_row(newest), ring_col(newest)
        if step > 0:
            later_n, later_w = pending_n, pending_w
        pending_n = long_row(newest) if step in row_sends else empty
        pending_w = long_col(newest) if step in col_sends else empty
    back = lax.dynamic_update_slice(back, swap(final), (batch - rows, 0))
    east_out = jnp.where(first, kept, back)
    west_out = jnp.where(first, back, kept)
    return east_out[None, None], west_out[None, None]


def solution(mesh):
    in_specs = (
        P("crow", "ccol", "half", None),
        P("crow", "ccol", None, "half"),
        P("crow", "ccol", None, "half"),
    )
    out_specs = (P("crow", "ccol", None, "half"), P("crow", "ccol", None, "half"))
    return jax.shard_map(local, mesh=mesh, in_specs=in_specs, out_specs=out_specs, check_vma=False)
```
